32 devices in a mesh: pipe: 2 (over x), tensor: 4 (over y, core), dp: 4 (over z).
Axes of the slice: x: 2, y: 2, z: 4, core: 2. Of those that a mesh axis runs over, the one named last changes fastest.
Arguments:
- inputs: bfloat16 [2, 512, 16384], P(None, 'dp', 'tensor'), may hold values from -6 to 6
- w_in: bfloat16 [2, 16384, 1024], P('pipe', ('tensor', 'dp')), may hold values from -0.046875 to 0.046875
- w_out: bfloat16 [2, 1024, 16384], P('pipe', None, ('tensor', 'dp')), may hold values from -0.1875 to 0.1875
- cotangent: bfloat16 [2, 512, 16384], P(None, 'dp', 'tensor'), may hold values from -6 to 6
Outputs:
- update_in: float32 [2, 16384, 1024], P('pipe', ('tensor', 'dp'))
- update_out: float32 [2, 1024, 16384], P('pipe', None, ('tensor', 'dp'))
- grad_norm: float32 [], replicated
The draws below stay inside these ranges and needn't reach their ends.
All inputs are finite; a program needn't handle non-finite values.
Results may differ from the reference program's by a relative error of at most 0.008.
Values may be sent and summed in bfloat16 or wider, within the bound.
A program may use at most 192 MiB of HBM per device.

```python
import jax
import jax.numpy as jnp
from jax import lax

D = 16384
H = 1024
MB = 2
TOK = 128
SECTIONS = 2
BATCH = 512
CLIP_NORM = 16384


def steps_of(key, dims, cuts, low, high):
    def one(dim, shards_of):
        draws = jax.random.uniform(jax.random.fold_in(jax.random.fold_in(key, 6), dim), (shards_of,), jnp.float32, low / len(cuts), high / len(cuts))
        return jnp.repeat(jnp.exp(draws), dims[dim] // shards_of).reshape((-1,) + (1,) * (len(dims) - dim - 1))

    gain = one(*cuts[0])
    for cut in cuts[1:]:
        gain = gain * one(*cut)
    return gain


def gaussian(key, extent, scale, most, split=(), dtype=jnp.bfloat16):
    gain = steps_of(key, extent, split, -0.22, 0.18) if split else 1.0
    values = jax.random.normal(key, extent, jnp.float32) * scale * gain
    return jnp.minimum(jnp.maximum(values, -most), most).astype(dtype)


def setup_inputs(seed: int = 0) -> dict:
    keys = jax.random.split(jax.random.key(seed), 5)
    return {
        "inputs": gaussian(keys[0], (MB, BATCH, D), 1.0, 6.0, ((1, 4), (2, 4))),
        "w_in": gaussian(keys[1], (SECTIONS, D, H), D ** -0.5, 0.046875, ((0, 2), (1, 16))),
        "w_out": gaussian(keys[2], (SECTIONS, H, D), H ** -0.5, 0.1875, ((0, 2), (2, 16))),
        "cotangent": gaussian(keys[3], (MB, BATCH, D), 1.0, 6.0, ((1, 4), (2, 4))),
    }


def silu_round(preact):
    return jax.nn.silu(preact).astype(jnp.bfloat16)

def slope_round(upward, preact):
    sigmoid_value = jax.nn.sigmoid(preact)
    return (upward * sigmoid_value * (1.0 + preact * (1.0 - sigmoid_value))).astype(jnp.bfloat16)

def kahan_add(running, carried, grad_term):
    corrected = grad_term - carried.astype(jnp.float32)
    summed = (running.astype(jnp.float32) + corrected).astype(jnp.bfloat16)
    carried = (summed.astype(jnp.float32) - running.astype(jnp.float32) - corrected).astype(jnp.bfloat16)
    return (summed, carried)

def reference(inputs, w_in, w_out, cotangent):
    replicas = BATCH // TOK
    stored_x = []
    stored_pre = []
    stored_act = []
    for micro_index in range(MB):
        current = inputs[micro_index]
        list_x, list_pre, list_act = ([], [], [])
        for layer in range(SECTIONS):
            preact = jnp.dot(current, w_in[layer], preferred_element_type=jnp.float32)
            activation = silu_round(preact)
            list_x.append(current)
            list_pre.append(preact)
            list_act.append(activation)
            current = (current.astype(jnp.float32) + jnp.dot(activation, w_out[layer], preferred_element_type=jnp.float32)).astype(jnp.bfloat16)
        stored_x.append(list_x)
        stored_pre.append(list_pre)
        stored_act.append(list_act)
    errors = [cotangent[micro_index] for micro_index in range(MB)]
    totals_in = [None] * SECTIONS
    totals_out = [None] * SECTIONS
    for layer in reversed(range(SECTIONS)):
        sum_in = jnp.zeros((replicas, D, H), jnp.bfloat16)
        err_in = jnp.zeros((replicas, D, H), jnp.bfloat16)
        sum_out = jnp.zeros((replicas, H, D), jnp.bfloat16)
        err_out = jnp.zeros((replicas, H, D), jnp.bfloat16)
        for micro_index in range(MB):
            upper = errors[micro_index]
            upward = jnp.dot(upper, w_out[layer].T, preferred_element_type=jnp.float32)
            slope = slope_round(upward, stored_pre[micro_index][layer])
            x_groups = stored_x[micro_index][layer].reshape(replicas, TOK, D).astype(jnp.float32)
            slope_groups = slope.reshape(replicas, TOK, H).astype(jnp.float32)
            act_groups = stored_act[micro_index][layer].reshape(replicas, TOK, H).astype(jnp.float32)
            err_groups = upper.reshape(replicas, TOK, D).astype(jnp.float32)
            grad_in = jnp.einsum('gtc,gth->gch', x_groups, slope_groups)
            grad_out = jnp.einsum('gth,gtc->ghc', act_groups, err_groups)
            sum_in, err_in = kahan_add(sum_in, err_in, grad_in)
            sum_out, err_out = kahan_add(sum_out, err_out, grad_out)
            errors[micro_index] = (upper.astype(jnp.float32) + jnp.dot(slope, w_in[layer].T, preferred_element_type=jnp.float32)).astype(jnp.bfloat16)
        totals_in[layer] = lax.optimization_barrier(jnp.sum(sum_in.astype(jnp.float32) - err_in.astype(jnp.float32), axis=0))
        totals_out[layer] = lax.optimization_barrier(jnp.sum(sum_out.astype(jnp.float32) - err_out.astype(jnp.float32), axis=0))
    total_in = jnp.stack(totals_in)
    total_out = jnp.stack(totals_out)
    grad_norm = jnp.sqrt(jnp.sum(total_in * total_in) + jnp.sum(total_out * total_out))
    factor = jnp.minimum(1.0, CLIP_NORM / grad_norm)
    return (total_in * factor, total_out * factor, grad_norm)
```

```python
import jax
import jax.numpy as jnp
from jax import lax
from jax.sharding import PartitionSpec as P

CLIP_NORM = 16384
BF = jnp.bfloat16
F32 = jnp.float32
PLANE = ("tensor", "dp")


def mm(a, b, ca, cb):
    return lax.dot_general(a, b, (((ca,), (cb,)), ((), ())), preferred_element_type=F32)


def swap_pipe(value):
    return lax.ppermute(value, "pipe", [(0, 1), (1, 0)])


def chain(a0, a1, u1, u0, g):
    act0 = jax.nn.silu(a0).astype(BF)
    pre1 = a1 + mm(act0, g, 1, 0)
    sig1 = jax.nn.sigmoid(pre1)
    act1 = (pre1 * sig1).astype(BF)
    slope1 = (u1 * sig1 * (1.0 + pre1 * (1.0 - sig1))).astype(BF)
    up0 = u0 + mm(slope1, g, 1, 1)
    sig0 = jax.nn.sigmoid(a0)
    slope0 = (up0 * sig0 * (1.0 + a0 * (1.0 - sig0))).astype(BF)
    return act0, act1, slope1, slope0


def on_device(inputs, w_in, w_out, cotangent):
    first = lax.axis_index("pipe") == 0
    a_own = w_in[0]
    b_own = w_out[0].T
    hidden = a_own.shape[1]
    v_other = swap_pipe(jnp.where(first, b_own, a_own))
    mine = lax.all_to_all(
        jnp.where(first, inputs, cotangent), "dp", split_axis=2, concat_axis=1, tiled=True
    )
    mine = mine.reshape(-1, mine.shape[-1])
    v_own = jnp.where(first, a_own, b_own)

    g_left = jnp.where(first, b_own, v_other)
    g_right = jnp.where(first, v_other, a_own)
    g_part = mm(g_left, g_right, 0, 0).astype(BF)
    g_share = lax.psum_scatter(g_part, PLANE, scatter_dimension=0, tiled=True)
    g = lax.all_gather(g_share, PLANE, axis=0, tiled=True)

    part = jnp.concatenate([mm(mine, v_own, 1, 0), mm(mine, v_other, 1, 0)], axis=1).astype(BF)
    share = lax.psum_scatter(part, PLANE, scatter_dimension=0, tiled=True)
    share_other = swap_pipe(share)
    other = swap_pipe(mine)
    pre_pair = jnp.where(first, share, share_other).astype(F32)
    up_pair = jnp.where(first, share_other, share).astype(F32)
    act0, act1, slope1, slope0 = chain(
        pre_pair[:, :hidden], pre_pair[:, hidden:], up_pair[:, :hidden], up_pair[:, hidden:], g
    )
    send = jnp.concatenate(
        [
            jnp.where(first, slope1, act0),
            jnp.where(first, act0, act1),
            jnp.where(first, slope0, slope1),
        ],
        axis=1,
    )
    full = lax.all_gather(send, PLANE, axis=0, tiled=True)
    relay, act, slope = full[:, :hidden], full[:, hidden : 2 * hidden], full[:, 2 * hidden :]
    moved = (other.astype(F32) + mm(relay, v_other, 1, 1)).astype(BF)
    x_here = jnp.where(first, mine, moved)
    err_here = jnp.where(first, moved, mine)
    total_in = mm(x_here, slope, 0, 0)
    total_out = mm(act, err_here, 0, 0)
    squares = jnp.sum(total_in * total_in) + jnp.sum(total_out * total_out)
    grad_norm = jnp.sqrt(lax.psum(squares, ("pipe", "tensor", "dp")))
    factor = jnp.minimum(1.0, CLIP_NORM / grad_norm)
    return ((total_in * factor)[None], (total_out * factor)[None], grad_norm)


def solution(mesh):
    in_specs = (
        P(None, "dp", "tensor"),
        P("pipe", ("tensor", "dp"), None),
        P("pipe", None, ("tensor", "dp")),
        P(None, "dp", "tensor"),
    )
    out_specs = (P("pipe", ("tensor", "dp"), None), P("pipe", None, ("tensor", "dp")), P())
    return jax.shard_map(
        on_device, mesh=mesh, in_specs=in_specs, out_specs=out_specs, check_vma=False
    )
```

```python
import jax
import jax.numpy as jnp
from jax import lax
from jax.experimental import pallas as pl
from jax.experimental.pallas import tpu as pltpu
from jax.sharding import PartitionSpec as P

CLIP_NORM = 16384
BF = jnp.bfloat16
F32 = jnp.float32


WIDTH = 512
BLOCK = 64
MESH = pl.DeviceIdType.MESH


def place():
    return tuple(lax.axis_index(name) for name in ("pipe", "tensor", "dp"))


def plane_peers():
    p, t, d = place()
    levels = lax.axis_size("tensor").bit_length() - 1
    count = lax.axis_size("dp")
    partners = []
    for level in range(levels):
        bit = 1 << level
        flipped = t + bit - 2 * bit * lax.rem(t // bit, 2)
        partners.append((p, flipped, d))
    ring = [(p, t, lax.rem(d + off, count)) for off in range(1, count)]
    back = [(p, t, lax.rem(d + count - off, count)) for off in range(1, count)]
    return partners, ring, back


def meet(peers):
    barrier = pltpu.get_barrier_semaphore()
    for peer in peers:
        pl.semaphore_signal(barrier, inc=1, device_id=peer, device_id_type=MESH)
    pl.semaphore_wait(barrier, len(peers))


def chunks_of(shapes):
    return [
        (item, pl.ds(col, min(WIDTH, shape[1])))
        for item, shape in enumerate(shapes)
        for col in range(0, shape[1], min(WIDTH, shape[1]))
    ]


def over_rows(rows, body):
    block = min(BLOCK, rows)

    def step(index, carry):
        body(pl.multiple_of(index * block, block), block)
        return carry

    lax.fori_loop(0, rows // block, step, 0)


def remote(src, dst, send_sem, recv_sem, peer):
    return pltpu.make_async_remote_copy(
        src_ref=src,
        dst_ref=dst,
        send_sem=send_sem,
        recv_sem=recv_sem,
        device_id=peer,
        device_id_type=MESH,
    )


def reduce_rows(parts, out_types, collective_id):
    shapes = [part.shape for part in parts]
    items = len(parts)
    levels = lax.axis_size("tensor").bit_length() - 1
    count = lax.axis_size("dp")
    ways = count << levels
    chunks = chunks_of(shapes)

    def kernel(*refs):
        ins, outs = refs[:items], refs[items : 2 * items]
        rest = refs[2 * items :]
        recvs = [rest[item * levels : (item + 1) * levels] for item in range(items)]
        rest = rest[items * levels :]
        sums = [rest[item * levels : (item + 1) * levels] for item in range(items)]
        rest = rest[items * levels :]
        lands = rest[:items]
        send_sem, recv_sem, ring_send, ring_recv = rest[items:]
        p, t, d = place()
        partners, ring, back = plane_peers()
        meet(partners + ring)
        sent = []

        def start(copy):
            copy.start()
            sent.append(copy)
            return copy

        def half(level, item):
            bit = lax.rem(t // (1 << level), 2)
            rows = shapes[item][0] >> (level + 1)
            return pl.multiple_of(bit * rows, rows), pl.multiple_of((1 - bit) * rows, rows), rows

        def exchange(level, slot):
            item, cols = chunks[slot]
            keep, give, rows = half(level, item)
            source = ins[item] if level == 0 else sums[item][level - 1]
            return start(
                remote(
                    source.at[pl.ds(give, rows), cols],
                    recvs[item][level].at[:, cols],
                    send_sem.at[level, slot],
                    recv_sem.at[level, slot],
                    partners[level],
                )
            )

        flight = [exchange(0, slot) for slot in range(len(chunks))]
        ringed = [None] * len(chunks)
        for level in range(levels):
            following = []
            for slot, (item, cols) in enumerate(chunks):
                keep, give, rows = half(level, item)
                source = ins[item] if level == 0 else sums[item][level - 1]
                flight[slot].wait_recv()

                def add(row, block, source=source, item=item, cols=cols, keep=keep):
                    left = source[pl.ds(pl.multiple_of(keep + row, block), block), cols]
                    right = recvs[item][level][pl.ds(row, block), cols]
                    total = left.astype(F32) + right.astype(F32)
                    sums[item][level][pl.ds(row, block), cols] = total.astype(BF)

                over_rows(rows, add)
                if level + 1 < levels:
                    following.append(exchange(level + 1, slot))
                else:
                    share = shapes[item][0] // ways
                    ringed[slot] = [
                        start(
                            remote(
                                sums[item][level].at[
                                    pl.ds(pl.multiple_of(peer[2] * share, share), share), cols
                                ],
                                lands[item].at[off, :, cols],
                                ring_send.at[off, slot],
                                ring_recv.at[off, slot],
                                peer,
                            )
                        )
                        for off, peer in enumerate(ring)
                    ]
            flight = following
        for slot, (item, cols) in enumerate(chunks):
            share = shapes[item][0] // ways
            for copy in ringed[slot]:
                copy.wait_recv()

            def finish(row, block, item=item, cols=cols, share=share):
                mine = pl.multiple_of(d * share + row, block)
                total = sums[item][levels - 1][pl.ds(mine, block), cols].astype(F32)
                for off in range(count - 1):
                    total = total + lands[item][off, pl.ds(row, block), cols].astype(F32)
                outs[item][pl.ds(row, block), cols] = total.astype(outs[item].dtype)

            over_rows(share, finish)
        for copy in sent:
            copy.wait_send()

    vmem = pl.BlockSpec(memory_space=pltpu.VMEM)
    halves = [
        pltpu.VMEM((shape[0] >> (level + 1), shape[1]), BF)
        for shape in shapes
        for level in range(levels)
    ]
    lands = [pltpu.VMEM((count - 1, shape[0] // ways, shape[1]), BF) for shape in shapes]
    dma = pltpu.SemaphoreType.DMA
    size = sum(part.size for part in parts)
    return pl.pallas_call(
        kernel,
        out_shape=[
            jax.ShapeDtypeStruct((shape[0] // ways, shape[1]), kind)
            for shape, kind in zip(shapes, out_types)
        ],
        in_specs=[vmem] * items,
        out_specs=[vmem] * items,
        scratch_shapes=halves
        + halves
        + lands
        + [
            dma((levels, len(chunks))),
            dma((levels, len(chunks))),
            dma((count - 1, len(chunks))),
            dma((count - 1, len(chunks))),
        ],
        compiler_params=pltpu.CompilerParams(
            collective_id=collective_id, has_side_effects=True, vmem_limit_bytes=64_000_000
        ),
        cost_estimate=pl.CostEstimate(flops=size, bytes_accessed=size * 40, transcendentals=0),
        name="reduce_rows",
    )(*parts)


def gather_rows(share_array, collective_id):
    share, width = share_array.shape
    levels = lax.axis_size("tensor").bit_length() - 1
    count = lax.axis_size("dp")
    rows_all = (share * count) << levels
    chunks = chunks_of([(rows_all, width)])

    def kernel(in_ref, out_ref, send_sem, recv_sem, ring_send, ring_recv, own_sem):
        p, t, d = place()
        partners, ring, back = plane_peers()
        meet(partners + ring)
        sent = []

        def start(copy):
            copy.start()
            sent.append(copy)
            return copy

        begin = [0]
        for level in range(levels):
            begin.append(begin[-1] + lax.rem(t // (1 << level), 2) * (rows_all >> (level + 1)))
        mine = pl.ds(pl.multiple_of(begin[levels] + d * share, share), share)
        local = pltpu.make_async_copy(in_ref, out_ref.at[mine, :], own_sem)
        local.start()
        flight = [
            [
                start(
                    remote(
                        in_ref.at[:, cols],
                        out_ref.at[mine, cols],
                        ring_send.at[off, slot],
                        ring_recv.at[off, slot],
                        peer,
                    )
                )
                for off, peer in enumerate(ring)
            ]
            for slot, (item, cols) in enumerate(chunks)
        ]
        local.wait()
        for level in reversed(range(levels)):
            rows = rows_all >> (level + 1)
            piece = pl.ds(pl.multiple_of(begin[level + 1], rows), rows)
            following = []
            for slot, (item, cols) in enumerate(chunks):
                for copy in flight[slot]:
                    copy.wait_recv()
                following.append(
                    [
                        start(
                            remote(
                                out_ref.at[piece, cols],
                                out_ref.at[piece, cols],
                                send_sem.at[level, slot],
                                recv_sem.at[level, slot],
                                partners[level],
                            )
                        )
                    ]
                )
            flight = following
        for copies in flight:
            for copy in copies:
                copy.wait_recv()
        for copy in sent:
            copy.wait_send()

    dma = pltpu.SemaphoreType.DMA
    size = rows_all * width
    return pl.pallas_call(
        kernel,
        out_shape=jax.ShapeDtypeStruct((rows_all, width), BF),
        in_specs=[pl.BlockSpec(memory_space=pltpu.VMEM)],
        out_specs=pl.BlockSpec(memory_space=pl.ANY),
        scratch_shapes=[
            dma((levels, len(chunks))),
            dma((levels, len(chunks))),
            dma((count - 1, len(chunks))),
            dma((count - 1, len(chunks))),
            dma,
        ],
        compiler_params=pltpu.CompilerParams(collective_id=collective_id, has_side_effects=True),
        cost_estimate=pl.CostEstimate(flops=size, bytes_accessed=size * 40, transcendentals=0),
        name="gather_rows",
    )(share_array)


def sum_all(value, collective_id):
    sizes = [lax.axis_size(name) for name in ("pipe", "tensor", "dp")]
    total = sizes[0] * sizes[1] * sizes[2]

    def kernel(in_ref, out_ref, land, send_sem, recv_sem):
        p, t, d = place()
        me = (p * sizes[1] + t) * sizes[2] + d

        def peer_of(off):
            there = lax.rem(me + off, total)
            return (
                there // (sizes[1] * sizes[2]),
                lax.rem(there // sizes[2], sizes[1]),
                lax.rem(there, sizes[2]),
            )

        def copy_of(off):
            return remote(
                in_ref, land.at[off - 1], send_sem.at[off - 1], recv_sem.at[off - 1], peer_of(off)
            )

        barrier = pltpu.get_barrier_semaphore()

        def greet(off, carry):
            pl.semaphore_signal(barrier, inc=1, device_id=peer_of(off), device_id_type=MESH)
            return carry

        lax.fori_loop(1, total, greet, 0)
        pl.semaphore_wait(barrier, total - 1)

        def send(off, carry):
            copy_of(off).start()
            return carry

        lax.fori_loop(1, total, send, 0)

        def receive(off, carry):
            copy_of(off).wait()
            return carry

        lax.fori_loop(1, total, receive, 0)
        out_ref[...] = in_ref[...] + jnp.sum(land[...], axis=0)

    vmem = pl.BlockSpec(memory_space=pltpu.VMEM)
    dma = pltpu.SemaphoreType.DMA
    return pl.pallas_call(
        kernel,
        out_shape=jax.ShapeDtypeStruct((8, 128), F32),
        in_specs=[vmem],
        out_specs=vmem,
        scratch_shapes=[pltpu.VMEM((total - 1, 8, 128), F32), dma((total - 1,)), dma((total - 1,))],
        compiler_params=pltpu.CompilerParams(collective_id=collective_id, has_side_effects=True),
        name="sum_all",
    )(jnp.full((8, 128), value, F32))[0, 0]


def mm(a, b, ca, cb):
    return lax.dot_general(a, b, (((ca,), (cb,)), ((), ())), preferred_element_type=F32)


def swap_pipe(value):
    return lax.ppermute(value, "pipe", [(0, 1), (1, 0)])


def chain(a0, a1, u1, u0, g):
    act0 = jax.nn.silu(a0).astype(BF)
    pre1 = a1 + mm(act0, g, 1, 0)
    sig1 = jax.nn.sigmoid(pre1)
    act1 = (pre1 * sig1).astype(BF)
    slope1 = (u1 * sig1 * (1.0 + pre1 * (1.0 - sig1))).astype(BF)
    up0 = u0 + mm(slope1, g, 1, 1)
    sig0 = jax.nn.sigmoid(a0)
    slope0 = (up0 * sig0 * (1.0 + a0 * (1.0 - sig0))).astype(BF)
    return act0, act1, slope1, slope0


def on_device(inputs, w_in, w_out, cotangent):
    first = lax.axis_index("pipe") == 0
    a_own = w_in[0]
    b_own = w_out[0].T
    hidden = a_own.shape[1]
    v_other = swap_pipe(jnp.where(first, b_own, a_own))
    mine = lax.all_to_all(
        jnp.where(first, inputs, cotangent), "dp", split_axis=2, concat_axis=1, tiled=True
    )
    mine = mine.reshape(-1, mine.shape[-1])
    v_own = jnp.where(first, a_own, b_own)

    g_left = jnp.where(first, b_own, v_other)
    g_right = jnp.where(first, v_other, a_own)
    g_part = mm(g_left, g_right, 0, 0).astype(BF)

    part = jnp.concatenate([mm(mine, v_own, 1, 0), mm(mine, v_other, 1, 0)], axis=1).astype(BF)
    g_share, share = reduce_rows([g_part, part], [BF, F32], 0)
    g = gather_rows(g_share, 1)
    share_other = swap_pipe(share.astype(BF)).astype(F32)
    other = swap_pipe(mine)
    pre_pair = jnp.where(first, share, share_other)
    up_pair = jnp.where(first, share_other, share)
    act0, act1, slope1, slope0 = chain(
        pre_pair[:, :hidden], pre_pair[:, hidden:], up_pair[:, :hidden], up_pair[:, hidden:], g
    )
    send = jnp.concatenate(
        [
            jnp.where(first, slope1, act0),
            jnp.where(first, act0, act1),
            jnp.where(first, slope0, slope1),
        ],
        axis=1,
    )
    full = gather_rows(send, 2)
    relay, act, slope = full[:, :hidden], full[:, hidden : 2 * hidden], full[:, 2 * hidden :]
    moved = (other.astype(F32) + mm(relay, v_other, 1, 1)).astype(BF)
    x_here = jnp.where(first, mine, moved)
    err_here = jnp.where(first, moved, mine)
    total_in = mm(x_here, slope, 0, 0)
    total_out = mm(act, err_here, 0, 0)
    squares = jnp.sum(total_in * total_in) + jnp.sum(total_out * total_out)
    grad_norm = jnp.sqrt(sum_all(squares, 3))
    factor = jnp.minimum(1.0, CLIP_NORM / grad_norm)
    return ((total_in * factor)[None], (total_out * factor)[None], grad_norm)


def solution(mesh):
    in_specs = (
        P(None, "dp", "tensor"),
        P("pipe", ("tensor", "dp"), None),
        P("pipe", None, ("tensor", "dp")),
        P(None, "dp", "tensor"),
    )
    out_specs = (P("pipe", ("tensor", "dp"), None), P("pipe", None, ("tensor", "dp")), P())
    return jax.shard_map(
        on_device, mesh=mesh, in_specs=in_specs, out_specs=out_specs, check_vma=False
    )
```

```python
import jax
import jax.numpy as jnp
from jax import lax
from jax.experimental import pallas as pl
from jax.experimental.pallas import tpu as pltpu
from jax.sharding import PartitionSpec as P

CLIP_NORM = 16384
BF = jnp.bfloat16
F32 = jnp.float32


WIDTH = 256
BLOCK = 64
MESH = pl.DeviceIdType.MESH


def place():
    return tuple(lax.axis_index(name) for name in ("pipe", "tensor", "dp"))


def plane_peers():
    p, t, d = place()
    levels = lax.axis_size("tensor").bit_length() - 1
    count = lax.axis_size("dp")
    partners = []
    for level in range(levels):
        bit = 1 << level
        flipped = t + bit - 2 * bit * lax.rem(t // bit, 2)
        partners.append((p, flipped, d))
    ring = [(p, t, lax.rem(d + off, count)) for off in range(1, count)]
    back = [(p, t, lax.rem(d + count - off, count)) for off in range(1, count)]
    return partners, ring, back


def meet(peers):
    barrier = pltpu.get_barrier_semaphore()
    for peer in peers:
        pl.semaphore_signal(barrier, inc=1, device_id=peer, device_id_type=MESH)
    pl.semaphore_wait(barrier, len(peers))


def chunks_of(shapes):
    return [
        (item, pl.ds(col, min(WIDTH, shape[1])))
        for item, shape in enumerate(shapes)
        for col in range(0, shape[1], min(WIDTH, shape[1]))
    ]


def over_rows(rows, body):
    block = min(BLOCK, rows)

    def step(index, carry):
        body(pl.multiple_of(index * block, block), block)
        return carry

    lax.fori_loop(0, rows // block, step, 0)


def remote(src, dst, send_sem, recv_sem, peer):
    return pltpu.make_async_remote_copy(
        src_ref=src,
        dst_ref=dst,
        send_sem=send_sem,
        recv_sem=recv_sem,
        device_id=peer,
        device_id_type=MESH,
    )


def reduce_rows(parts, out_types, collective_id):
    shapes = [part.shape for part in parts]
    items = len(parts)
    levels = lax.axis_size("tensor").bit_length() - 1
    count = lax.axis_size("dp")
    ways = count << levels
    chunks = chunks_of(shapes)

    def kernel(*refs):
        ins, outs = refs[:items], refs[items : 2 * items]
        rest = refs[2 * items :]
        recvs = [rest[item * levels : (item + 1) * levels] for item in range(items)]
        rest = rest[items * levels :]
        sums = [rest[item * levels : (item + 1) * levels] for item in range(items)]
        rest = rest[items * levels :]
        lands = rest[:items]
        send_sem, recv_sem, ring_send, ring_recv = rest[items:]
        p, t, d = place()
        partners, ring, back = plane_peers()
        meet(partners + ring)
        sent = []

        def start(copy):
            copy.start()
            sent.append(copy)
            return copy

        def half(level, item):
            bit = lax.rem(t // (1 << level), 2)
            rows = shapes[item][0] >> (level + 1)
            return pl.multiple_of(bit * rows, rows), pl.multiple_of((1 - bit) * rows, rows), rows

        def exchange(level, slot):
            item, cols = chunks[slot]
            keep, give, rows = half(level, item)
            source = ins[item] if level == 0 else sums[item][level - 1]
            return start(
                remote(
                    source.at[pl.ds(give, rows), cols],
                    recvs[item][level].at[:, cols],
                    send_sem.at[level, slot],
                    recv_sem.at[level, slot],
                    partners[level],
                )
            )

        flight = [exchange(0, slot) for slot in range(len(chunks))]
        ringed = [None] * len(chunks)
        for level in range(levels):
            following = []
            for slot, (item, cols) in enumerate(chunks):
                keep, give, rows = half(level, item)
                source = ins[item] if level == 0 else sums[item][level - 1]
                flight[slot].wait_recv()

                def add(row, block, source=source, item=item, cols=cols, keep=keep):
                    left = source[pl.ds(pl.multiple_of(keep + row, block), block), cols]
                    right = recvs[item][level][pl.ds(row, block), cols]
                    total = left.astype(F32) + right.astype(F32)
                    sums[item][level][pl.ds(row, block), cols] = total.astype(BF)

                over_rows(rows, add)
                if level + 1 < levels:
                    following.append(exchange(level + 1, slot))
                else:
                    share = shapes[item][0] // ways
                    ringed[slot] = [
                        start(
                            remote(
                                sums[item][level].at[
                                    pl.ds(pl.multiple_of(peer[2] * share, share), share), cols
                                ],
                                lands[item].at[off, :, cols],
                                ring_send.at[off, slot],
                                ring_recv.at[off, slot],
                                peer,
                            )
                        )
                        for off, peer in enumerate(ring)
                    ]
            flight = following
        for slot, (item, cols) in enumerate(chunks):
            share = shapes[item][0] // ways
            for copy in ringed[slot]:
                copy.wait_recv()

            def finish(row, block, item=item, cols=cols, share=share):
                mine = pl.multiple_of(d * share + row, block)
                total = sums[item][levels - 1][pl.ds(mine, block), cols].astype(F32)
                for off in range(count - 1):
                    total = total + lands[item][off, pl.ds(row, block), cols].astype(F32)
                outs[item][pl.ds(row, block), cols] = total.astype(outs[item].dtype)

            over_rows(share, finish)
        for copy in sent:
            copy.wait_send()

    vmem = pl.BlockSpec(memory_space=pltpu.VMEM)
    halves = [
        pltpu.VMEM((shape[0] >> (level + 1), shape[1]), BF)
        for shape in shapes
        for level in range(levels)
    ]
    lands = [pltpu.VMEM((count - 1, shape[0] // ways, shape[1]), BF) for shape in shapes]
    dma = pltpu.SemaphoreType.DMA
    size = sum(part.size for part in parts)
    return pl.pallas_call(
        kernel,
        out_shape=[
            jax.ShapeDtypeStruct((shape[0] // ways, shape[1]), kind)
            for shape, kind in zip(shapes, out_types)
        ],
        in_specs=[vmem] * items,
        out_specs=[vmem] * items,
        scratch_shapes=halves
        + halves
        + lands
        + [
            dma((levels, len(chunks))),
            dma((levels, len(chunks))),
            dma((count - 1, len(chunks))),
            dma((count - 1, len(chunks))),
        ],
        compiler_params=pltpu.CompilerParams(
            collective_id=collective_id, has_side_effects=True, vmem_limit_bytes=64_000_000
        ),
        cost_estimate=pl.CostEstimate(flops=size, bytes_accessed=size * 40, transcendentals=0),
        name="reduce_rows",
    )(*parts)


def gather_rows(share_array, collective_id):
    share, width = share_array.shape
    levels = lax.axis_size("tensor").bit_length() - 1
    count = lax.axis_size("dp")
    rows_all = (share * count) << levels
    chunks = chunks_of([(rows_all, width)])

    def kernel(in_ref, out_ref, send_sem, recv_sem, ring_send, ring_recv, own_sem):
        p, t, d = place()
        partners, ring, back = plane_peers()
        meet(partners + ring)
        sent = []

        def start(copy):
            copy.start()
            sent.append(copy)
            return copy

        begin = [0]
        for level in range(levels):
            begin.append(begin[-1] + lax.rem(t // (1 << level), 2) * (rows_all >> (level + 1)))
        mine = pl.ds(pl.multiple_of(begin[levels] + d * share, share), share)
        local = pltpu.make_async_copy(in_ref, out_ref.at[mine, :], own_sem)
        local.start()
        flight = [
            [
                start(
                    remote(
                        in_ref.at[:, cols],
                        out_ref.at[mine, cols],
                        ring_send.at[off, slot],
                        ring_recv.at[off, slot],
                        peer,
                    )
                )
                for off, peer in enumerate(ring)
            ]
            for slot, (item, cols) in enumerate(chunks)
        ]
        local.wait()
        for level in reversed(range(levels)):
            rows = rows_all >> (level + 1)
            piece = pl.ds(pl.multiple_of(begin[level + 1], rows), rows)
            following = []
            for slot, (item, cols) in enumerate(chunks):
                for copy in flight[slot]:
                    copy.wait_recv()
                following.append(
                    [
                        start(
                            remote(
                                out_ref.at[piece, cols],
                                out_ref.at[piece, cols],
                                send_sem.at[level, slot],
                                recv_sem.at[level, slot],
                                partners[level],
                            )
                        )
                    ]
                )
            flight = following
        for copies in flight:
            for copy in copies:
                copy.wait_recv()
        for copy in sent:
            copy.wait_send()

    dma = pltpu.SemaphoreType.DMA
    size = rows_all * width
    return pl.pallas_call(
        kernel,
        out_shape=jax.ShapeDtypeStruct((rows_all, width), BF),
        in_specs=[pl.BlockSpec(memory_space=pltpu.VMEM)],
        out_specs=pl.BlockSpec(memory_space=pl.ANY),
        scratch_shapes=[
            dma((levels, len(chunks))),
            dma((levels, len(chunks))),
            dma((count - 1, len(chunks))),
            dma((count - 1, len(chunks))),
            dma,
        ],
        compiler_params=pltpu.CompilerParams(collective_id=collective_id, has_side_effects=True),
        cost_estimate=pl.CostEstimate(flops=size, bytes_accessed=size * 40, transcendentals=0),
        name="gather_rows",
    )(share_array)


def sum_all(value, collective_id):
    sizes = [lax.axis_size(name) for name in ("pipe", "tensor", "dp")]
    total = sizes[0] * sizes[1] * sizes[2]

    def kernel(in_ref, out_ref, land, send_sem, recv_sem):
        p, t, d = place()
        me = (p * sizes[1] + t) * sizes[2] + d

        def peer_of(off):
            there = lax.rem(me + off, total)
            return (
                there // (sizes[1] * sizes[2]),
                lax.rem(there // sizes[2], sizes[1]),
                lax.rem(there, sizes[2]),
            )

        def copy_of(off):
            return remote(
                in_ref, land.at[off - 1], send_sem.at[off - 1], recv_sem.at[off - 1], peer_of(off)
            )

        barrier = pltpu.get_barrier_semaphore()

        def greet(off, carry):
            pl.semaphore_signal(barrier, inc=1, device_id=peer_of(off), device_id_type=MESH)
            return carry

        lax.fori_loop(1, total, greet, 0)
        pl.semaphore_wait(barrier, total - 1)

        def send(off, carry):
            copy_of(off).start()
            return carry

        lax.fori_loop(1, total, send, 0)

        def receive(off, carry):
            copy_of(off).wait()
            return carry

        lax.fori_loop(1, total, receive, 0)
        out_ref[...] = in_ref[...] + jnp.sum(land[...], axis=0)

    vmem = pl.BlockSpec(memory_space=pltpu.VMEM)
    dma = pltpu.SemaphoreType.DMA
    return pl.pallas_call(
        kernel,
        out_shape=jax.ShapeDtypeStruct((8, 128), F32),
        in_specs=[vmem],
        out_specs=vmem,
        scratch_shapes=[pltpu.VMEM((total - 1, 8, 128), F32), dma((total - 1,)), dma((total - 1,))],
        compiler_params=pltpu.CompilerParams(collective_id=collective_id, has_side_effects=True),
        name="sum_all",
    )(jnp.full((8, 128), value, F32))[0, 0]


def spread(inputs, cotangent, weight, collective_id):
    count = lax.axis_size("dp")
    batches, tokens, width = inputs.shape
    part = width // count

    def kernel(in_ref, cot_ref, w_ref, out_ref, far_ref, send_sem, recv_sem, w_send, w_recv, own_sem):
        p, t, d = place()
        partners, ring, back = plane_peers()
        across = (1 - p, t, d)
        meet(ring + [across])

        def columns(index):
            return pl.ds(pl.multiple_of(index * part, part), part)

        def copies_of(source):
            return [
                remote(
                    source.at[:, :, columns(peer[2])],
                    out_ref.at[d],
                    send_sem.at[off],
                    recv_sem.at[off],
                    peer,
                )
                for off, peer in enumerate(ring)
            ]

        def own_of(source):
            return pltpu.make_async_copy(source.at[:, :, columns(d)], out_ref.at[d], own_sem)

        def begin(source):
            for copy in copies_of(source):
                copy.start()
            own_of(source).start()

        weights = remote(w_ref, far_ref, w_send, w_recv, across)
        weights.start()

        @pl.when(p == 0)
        def _():
            begin(in_ref)

        @pl.when(p != 0)
        def _():
            begin(cot_ref)

        for copy in copies_of(in_ref):
            copy.wait()
        own_of(in_ref).wait()
        weights.wait()

    anywhere = pl.BlockSpec(memory_space=pl.ANY)
    dma = pltpu.SemaphoreType.DMA
    return pl.pallas_call(
        kernel,
        out_shape=[
            jax.ShapeDtypeStruct((count, batches, tokens, part), BF),
            jax.ShapeDtypeStruct(weight.shape, BF),
        ],
        in_specs=[anywhere] * 3,
        out_specs=[anywhere] * 2,
        scratch_shapes=[dma((count - 1,)), dma((count - 1,)), dma, dma, dma],
        compiler_params=pltpu.CompilerParams(collective_id=collective_id, has_side_effects=True),
        cost_estimate=pl.CostEstimate(
            flops=inputs.size, bytes_accessed=inputs.size * 40, transcendentals=0
        ),
        name="spread",
    )(inputs, cotangent, weight)


def mm(a, b, ca, cb):
    return lax.dot_general(a, b, (((ca,), (cb,)), ((), ())), preferred_element_type=F32)


def swap_pipe(value):
    return lax.ppermute(value, "pipe", [(0, 1), (1, 0)])


def chain(a0, a1, u1, u0, g):
    act0 = jax.nn.silu(a0).astype(BF)
    pre1 = a1 + mm(act0, g, 1, 0)
    sig1 = jax.nn.sigmoid(pre1)
    act1 = (pre1 * sig1).astype(BF)
    slope1 = (u1 * sig1 * (1.0 + pre1 * (1.0 - sig1))).astype(BF)
    up0 = u0 + mm(slope1, g, 1, 1)
    sig0 = jax.nn.sigmoid(a0)
    slope0 = (up0 * sig0 * (1.0 + a0 * (1.0 - sig0))).astype(BF)
    return act0, act1, slope1, slope0


def on_device(inputs, w_in, w_out, cotangent):
    first = lax.axis_index("pipe") == 0
    a_own = w_in[0]
    b_own = w_out[0].T
    hidden = a_own.shape[1]
    mine, v_other = spread(inputs, cotangent, jnp.where(first, b_own, a_own), 4)
    mine = mine.reshape(-1, mine.shape[-1])
    v_own = jnp.where(first, a_own, b_own)

    g_left = jnp.where(first, b_own, v_other)
    g_right = jnp.where(first, v_other, a_own)
    g_part = mm(g_left, g_right, 0, 0).astype(BF)

    part = jnp.concatenate([mm(mine, v_own, 1, 0), mm(mine, v_other, 1, 0)], axis=1).astype(BF)
    g_share, share = reduce_rows([g_part, part], [BF, F32], 0)
    g = gather_rows(g_share, 1)
    share_other = swap_pipe(share.astype(BF)).astype(F32)
    other = swap_pipe(mine)
    pre_pair = jnp.where(first, share, share_other)
    up_pair = jnp.where(first, share_other, share)
    act0, act1, slope1, slope0 = chain(
        pre_pair[:, :hidden], pre_pair[:, hidden:], up_pair[:, :hidden], up_pair[:, hidden:], g
    )
    send = jnp.concatenate(
        [
            jnp.where(first, slope1, act0),
            jnp.where(first, act0, act1),
            jnp.where(first, slope0, slope1),
        ],
        axis=1,
    )
    full = gather_rows(send, 2)
    relay, act, slope = full[:, :hidden], full[:, hidden : 2 * hidden], full[:, 2 * hidden :]
    moved = (other.astype(F32) + mm(relay, v_other, 1, 1)).astype(BF)
    x_here = jnp.where(first, mine, moved)
    err_here = jnp.where(first, moved, mine)
    total_in = mm(x_here, slope, 0, 0)
    total_out = mm(act, err_here, 0, 0)
    squares = jnp.sum(total_in * total_in) + jnp.sum(total_out * total_out)
    grad_norm = jnp.sqrt(sum_all(squares, 3))
    factor = jnp.minimum(1.0, CLIP_NORM / grad_norm)
    return ((total_in * factor)[None], (total_out * factor)[None], grad_norm)


def solution(mesh):
    in_specs = (
        P(None, "dp", "tensor"),
        P("pipe", ("tensor", "dp"), None),
        P("pipe", None, ("tensor", "dp")),
        P(None, "dp", "tensor"),
    )
    out_specs = (P("pipe", ("tensor", "dp"), None), P("pipe", None, ("tensor", "dp")), P())
    return jax.shard_map(
        on_device, mesh=mesh, in_specs=in_specs, out_specs=out_specs, check_vma=False
    )
```
